32 devices in a mesh: gx: 4 (over y, x), gy: 8 (over z, core).
Axes of the slice: x: 2, y: 2, z: 4, core: 2. Of those that a mesh axis runs over, the one named last changes fastest.
Arguments:
- density_one: float32 [512, 512, 512], P('gx', 'gy'), may hold values from -6 to 6
- density_two: float32 [512, 512, 512], P('gx', 'gy'), may hold values from -6 to 6
Outputs:
- correlation: float32 [512, 512, 512], P('gx', 'gy')
The draws below stay inside these ranges and needn't reach their ends.
All inputs are finite; a program needn't handle non-finite values.
Results may differ from the reference program's by a relative error of at most 0.00013.
Values sent between devices are 32-bit elements; how exact they have to be, the bound alone decides.
No kernel may reach another device: no remote copies, remote signals or barrier semaphores. Data moves between devices by JAX's collectives and lax.ppermute only.
A program may use at most 256 MiB of HBM per device.

```python
import math
import jax
import jax.numpy as jnp

NX = 512
NY = 512
NZ = 512


def levels(stream_key, extent, pieces, low, largest):
    def one(position, parts):
        steps = jax.random.uniform(jax.random.fold_in(jax.random.fold_in(stream_key, 6), position), (parts,), jnp.float32, low / len(pieces), largest / len(pieces))
        return jnp.repeat(jnp.exp(steps), extent[position] // parts).reshape((-1,) + (1,) * (len(extent) - position - 1))

    level = one(*pieces[0])
    for cut in pieces[1:]:
        level = level * one(*cut)
    return level


def normal_values(own_key, extent, scale, reach, cuts=(), kind=jnp.bfloat16):
    result = scale * jax.random.normal(own_key, extent, jnp.float32)
    if cuts:
        result = result * levels(own_key, extent, cuts, -0.22, 0.18)
    return jnp.clip(result, -reach, reach).astype(kind)


def setup_inputs(seed: int = 0) -> dict:
    arg_keys = jax.random.split(jax.random.key(seed), 3)
    return {
        "density_one": normal_values(arg_keys[0], (NX, NY, NZ), 1.0, 6.0, ((0, 4), (1, 8)), jnp.float32),
        "density_two": normal_values(arg_keys[1], (NX, NY, NZ), 1.0, 6.0, ((0, 4), (1, 8)), jnp.float32),
    }


def reference(density_one, density_two):
    cell_total = NX * NY * NZ
    spectrum_one = jnp.fft.rfftn(density_one)
    spectrum_two = jnp.fft.rfftn(density_two)
    power = (spectrum_one.real * spectrum_two.real + spectrum_one.imag * spectrum_two.imag) / cell_total
    wave_x = jnp.arange(NX)[:, None, None]
    wave_y = jnp.arange(NY)[None, :, None]
    wave_z = jnp.arange(NZ // 2 + 1)[None, None, :]
    kept_modes = (wave_x != NX // 2) & (wave_y != NY // 2) & (wave_z != NZ // 2)
    power = jnp.where(kept_modes, power, jnp.zeros_like(power))
    correlation = jnp.fft.irfftn(power * (1.0 + 0j), s=(NX, NY, NZ)) * math.sqrt(cell_total)
    return correlation.astype(jnp.float32)
```

```python
import math

import jax
import jax.numpy as jnp
from jax import lax
from jax.experimental import pallas as pl
from jax.experimental.pallas import tpu as pltpu
from jax.sharding import PartitionSpec as P

exact_mode = lax.Precision.HIGHEST


def phases(numerator, denominator):
    radians = (numerator % denominator).astype(jnp.float32) * (2.0 * math.pi / denominator)
    return (jnp.cos(radians), jnp.sin(radians))


def complex_table(length, direction):
    positions = jnp.arange(length, dtype=jnp.int32)
    cosines, sines_raw = phases(positions[:, None] * positions[None, :], length)
    signed = direction * sines_raw
    real_rows = jnp.stack([cosines, signed], axis=1)
    imag_rows = jnp.stack([-signed, cosines], axis=1)
    return jnp.stack([real_rows, imag_rows], axis=0)


def depth_tables(depth_cells, count_x, count_y):
    half_depth = depth_cells // 2
    kz_slices = half_depth // (count_x * count_y)
    row_ids = jnp.arange(2 * half_depth, dtype=jnp.int32)
    within = row_ids % kz_slices
    imag_flag = row_ids // kz_slices % 2
    row_block = row_ids // (2 * kz_slices)
    row_block = row_block % count_y * count_x + row_block // count_y
    wave_number = row_block * kz_slices + within
    cell_ids = jnp.arange(depth_cells, dtype=jnp.int32)
    cosines, sines_raw = phases(wave_number[:, None] * cell_ids[None, :], depth_cells)
    is_imag = (imag_flag == 1)[:, None]
    forward = jnp.where(is_imag, -sines_raw, cosines)
    weight = jnp.where(wave_number == 0, 1.0, 2.0)[:, None]
    inverse = jnp.where(is_imag, -weight * sines_raw, weight * cosines)
    return (forward, inverse)


def generic_device(density_one, density_two):
    count_x = lax.axis_size("gx")
    count_y = lax.axis_size("gy")
    x_local, y_local, depth_cells = density_one.shape
    grid_x = x_local * count_x
    grid_y = y_local * count_y
    kz_slices = depth_cells // 2 // (count_x * count_y)
    columns = x_local * y_local
    cell_total = float(grid_x * grid_y * depth_cells)
    forward_depth, inverse_depth = depth_tables(depth_cells, count_x, count_y)

    def depth_forward(density):
        flat_lines = density.reshape(columns, depth_cells)
        return lax.dot_general(
            forward_depth, flat_lines, (((1,), (1,)), ((), ())), precision=exact_mode
        )

    spectra = jnp.stack([depth_forward(density_one), depth_forward(density_two)])
    y_forward = complex_table(grid_y, -1.0).reshape(2, count_y, y_local, 2, grid_y)
    y_inverse = complex_table(grid_y, 1.0).reshape(2, grid_y, 2, count_y, y_local)
    block_forward = complex_table(count_x, -1.0)
    block_inverse = complex_table(count_x, 1.0)
    local_forward = complex_table(x_local, -1.0)
    sent = spectra.reshape(2, count_x * count_y, 2 * kz_slices, columns)
    moved = lax.all_to_all(sent, ("gx", "gy"), split_axis=1, concat_axis=1, tiled=True)
    moved = moved.reshape(2, count_x, count_y, 2, kz_slices, x_local, y_local)
    planes = jnp.einsum("fdspkjy,psyrq->fdrkjq", moved, y_forward, precision=exact_mode)
    aligned = jnp.einsum("fdpkjq,pdra->farkjq", planes, block_forward, precision=exact_mode)
    twiddle_cos, twiddle_sin = phases(
        jnp.arange(count_x, dtype=jnp.int32)[:, None]
        * jnp.arange(x_local, dtype=jnp.int32)[None, :],
        grid_x,
    )
    forward_cos = twiddle_cos[None, :, None, :, None]
    forward_sin = twiddle_sin[None, :, None, :, None]
    real_part = aligned[:, :, 0]
    imag_part = aligned[:, :, 1]
    turned = jnp.stack(
        [
            real_part * forward_cos + imag_part * forward_sin,
            imag_part * forward_cos - real_part * forward_sin,
        ],
        axis=2,
    )
    spectra_k = jnp.einsum("fapkjq,pjrb->farkbq", turned, local_forward, precision=exact_mode)
    power = (
        spectra_k[0, :, 0] * spectra_k[1, :, 0] + spectra_k[0, :, 1] * spectra_k[1, :, 1]
    ) / cell_total
    wave_x = (
        jnp.arange(count_x, dtype=jnp.int32)[:, None]
        + count_x * jnp.arange(x_local, dtype=jnp.int32)[None, :]
    )
    keep_x = (wave_x != grid_x // 2)[:, None, :, None]
    keep_y = (jnp.arange(grid_y, dtype=jnp.int32) != grid_y // 2)[None, None, None, :]
    power = jnp.where(keep_x & keep_y, power, 0.0)
    cos_local, sin_local = phases(
        jnp.arange(x_local, dtype=jnp.int32)[:, None]
        * jnp.arange(x_local, dtype=jnp.int32)[None, :],
        x_local,
    )
    real_table = jnp.stack([cos_local, sin_local], axis=1)
    lines = jnp.einsum("akbq,brj->arkjq", power, real_table, precision=exact_mode)
    inverse_cos = twiddle_cos[:, None, :, None]
    inverse_sin = twiddle_sin[:, None, :, None]
    real_part = lines[:, 0]
    imag_part = lines[:, 1]
    unturned = jnp.stack(
        [
            real_part * inverse_cos - imag_part * inverse_sin,
            imag_part * inverse_cos + real_part * inverse_sin,
        ],
        axis=1,
    )[None]
    blocks = jnp.einsum("fapkjq,pard->fdrkjq", unturned, block_inverse, precision=exact_mode)
    back_lines = jnp.einsum("fdpkjq,pqrsy->fdsrkjy", blocks, y_inverse, precision=exact_mode)
    sent_back = back_lines.reshape(1, count_x * count_y, 2 * kz_slices, columns)
    rows_back = lax.all_to_all(sent_back, ("gx", "gy"), split_axis=1, concat_axis=1, tiled=True)
    rows_flat = rows_back.reshape(2 * kz_slices * count_x * count_y, columns)
    correlation = lax.dot_general(
        rows_flat, inverse_depth, (((0,), (0,)), ((), ())), precision=exact_mode
    )
    correlation = correlation * (1.0 / math.sqrt(cell_total))
    return correlation.reshape(x_local, y_local, depth_cells)


VMEM_LIMIT = 60 * 1024 * 1024
MAX_CHUNKS = 2
Y_BLOCK = 8


def split(value):
    high = value.astype(jnp.bfloat16)
    low = (value - high.astype(jnp.float32)).astype(jnp.bfloat16)
    return high, low


def dot3(left_high, left_low, right_high, right_low):
    def one(a, b):
        return jnp.dot(a, b, preferred_element_type=jnp.float32)

    return one(left_high, right_high) + one(left_high, right_low) + one(left_low, right_high)


def cosine_pair(steps, length, factor=None):
    turned = jnp.cos((steps % length).astype(jnp.float32) * (2.0 * math.pi / length))
    if factor is not None:
        turned = turned * factor
    high = lax.reduce_precision(turned, 8, 7)
    return high.astype(jnp.bfloat16), (turned - high).astype(jnp.bfloat16)


def depth_rows(chunk, chunks, devices, kz_slices):
    per_chunk = kz_slices // chunks
    rows = jnp.arange(devices * 2 * per_chunk, dtype=jnp.int32)
    device = rows // (2 * per_chunk)
    flag = rows // per_chunk % 2
    return device * kz_slices + chunk * per_chunk + rows % per_chunk, flag


def depth_forward_kernel(one_ref, two_ref, high_ref, low_ref, out_ref, turn_ref):
    x_local, y_block, depth = one_ref.shape
    rows = high_ref.shape[1]
    lines = x_local * y_block
    step = min(256, lines)
    group = out_ref.shape[2] * out_ref.shape[3]
    flat_out = out_ref.reshape(2 * rows * y_block, x_local)
    for field, ref in enumerate((one_ref, two_ref)):
        flat = ref.reshape(lines, depth)

        def multiply(i, carry):
            high, low = split(flat[pl.ds(i * step, step), :])
            product = dot3(high, low, high_ref[...], low_ref[...])
            for part in range(rows // 128):
                turn_ref[field, part, pl.ds(i * step, step), :] = product[:, part * 128 : part * 128 + 128]
            return carry

        lax.fori_loop(0, lines // step, multiply, 0)
    for field in range(2):
        for part in range(rows // 128):
            lanes = turn_ref.at[field, part]
            for j in range(y_block):
                block = lanes[pl.ds(j, x_local, stride=y_block), :]
                turned = block.T
                for d in range(128 // group):
                    start = (2 * (part * (128 // group) + d) + field) * group * y_block + j
                    flat_out[pl.ds(start, group, stride=y_block), :] = turned[d * group : d * group + group]


def depth_forward(one, two, table, rows_shape):
    x_local, y_local, depth = one.shape
    rows = math.prod(rows_shape)
    out_rows = (rows_shape[0], 2, *rows_shape[1:])
    field_spec = pl.BlockSpec((x_local, Y_BLOCK, depth), lambda i: (0, i, 0))
    table_spec = pl.BlockSpec((depth, rows), lambda i: (0, 0))
    return pl.pallas_call(
        depth_forward_kernel,
        grid=(y_local // Y_BLOCK,),
        in_specs=[field_spec, field_spec, table_spec, table_spec],
        out_specs=pl.BlockSpec((*out_rows, Y_BLOCK, x_local), lambda i: (0, 0, 0, 0, i, 0)),
        out_shape=jax.ShapeDtypeStruct((*out_rows, y_local, x_local), jnp.float32),
        scratch_shapes=[pltpu.VMEM((2, rows // 128, x_local * Y_BLOCK, 128), jnp.float32)],
        compiler_params=pltpu.CompilerParams(vmem_limit_bytes=VMEM_LIMIT),
        name="depth_forward",
    )(one, two, *table)


def depth_inverse_kernel(*refs):
    *part_refs, high_ref, low_ref, out_ref, turn_ref = refs
    x_local, y_block, depth = out_ref.shape
    lines = x_local * y_block
    blocks = 0
    for part_ref in part_refs:
        rows = part_ref.shape[0] * part_ref.shape[1] * part_ref.shape[2]
        flat = part_ref.reshape(rows * y_block, x_local)
        for part in range(rows // 128):
            for j in range(y_block):
                block = flat[pl.ds(part * 128 * y_block + j, 128, stride=y_block), :]
                turn_ref[blocks, pl.ds(j, x_local, stride=y_block), :] = block.T
            blocks += 1
    step = min(256, lines)
    flat_out = out_ref.reshape(lines, depth)

    def multiply(i, carry):
        window = pl.ds(i * step, step)
        left = jnp.concatenate([turn_ref[b, window, :] for b in range(blocks)], axis=1)
        high, low = split(left)
        flat_out[window, :] = dot3(high, low, high_ref[...], low_ref[...])
        return carry

    lax.fori_loop(0, lines // step, multiply, 0)


def depth_inverse(parts, table):
    devices, two, kz_chunk, y_local, x_local = parts[0].shape
    rows, depth = table[0].shape
    part_spec = pl.BlockSpec((devices, two, kz_chunk, Y_BLOCK, x_local), lambda i: (0, 0, 0, i, 0))
    table_spec = pl.BlockSpec((rows, depth), lambda i: (0, 0))
    return pl.pallas_call(
        depth_inverse_kernel,
        grid=(y_local // Y_BLOCK,),
        in_specs=[part_spec] * len(parts) + [table_spec, table_spec],
        out_specs=pl.BlockSpec((x_local, Y_BLOCK, depth), lambda i: (0, i, 0)),
        out_shape=jax.ShapeDtypeStruct((x_local, y_local, depth), jnp.float32),
        scratch_shapes=[pltpu.VMEM((rows // 128, x_local * Y_BLOCK, 128), jnp.float32)],
        compiler_params=pltpu.CompilerParams(vmem_limit_bytes=VMEM_LIMIT),
        name="depth_inverse",
    )(*parts, *table)


def plane_kernel(
    s_ref, wy_high, wy_low, wx_high, wx_low, vx_high, vx_low, vy_high, vy_low, out_ref,
    s_high, s_low, y_high, y_low, p_high, p_low, g_high, g_low, *, count_x, count_y, tile, scale,
):
    y_local, x_local = out_ref.shape[-2:]
    grid_x, grid_y = count_x * x_local, count_y * y_local
    pair = 2 * y_local

    def load(i, carry):
        field, row = i // count_y, i % count_y
        for g in range(count_x):
            values = s_ref[g * count_y + row, field].reshape(pair, x_local)
            high, low = split(values)
            here = (field, pl.ds(row * pair, pair), slice(g * x_local, (g + 1) * x_local))
            s_high[here] = high
            s_low[here] = low
        return carry

    lax.fori_loop(0, 2 * count_y, load, 0)

    def middle(t, carry):
        rows = pl.ds(t * 2 * tile, 2 * tile)
        for field in range(2):
            for b in range(grid_x // 256):
                columns = slice(b * 256, b * 256 + 256)
                planes = dot3(
                    wy_high[rows, :], wy_low[rows, :], s_high[field, :, columns], s_low[field, :, columns]
                )
                high, low = split(planes)
                for r in range(2):
                    lanes = slice(r * grid_x + b * 256, r * grid_x + b * 256 + 256)
                    y_high[field * tile : (field + 1) * tile, lanes] = high[r * tile : (r + 1) * tile]
                    y_low[field * tile : (field + 1) * tile, lanes] = low[r * tile : (r + 1) * tile]
        for b in range(grid_x // 256):
            power = None
            for r in range(2):
                columns = slice(r * grid_x + b * 256, r * grid_x + b * 256 + 256)
                z = dot3(y_high[...], y_low[...], wx_high[:, columns], wx_low[:, columns])
                term = z[:tile] * z[tile:]
                power = term if power is None else power + term
            wave_y = t * tile + lax.broadcasted_iota(jnp.int32, power.shape, 0)
            wave_x = b * 256 + lax.broadcasted_iota(jnp.int32, power.shape, 1)
            keep = (wave_x != grid_x // 2) & (wave_y != grid_y // 2)
            high, low = split(jnp.where(keep, power * scale, 0.0))
            p_high[:, b * 256 : b * 256 + 256] = high
            p_low[:, b * 256 : b * 256 + 256] = low
        for r in range(2):
            for b in range(grid_x // 256):
                columns = slice(r * grid_x + b * 256, r * grid_x + b * 256 + 256)
                lines = dot3(p_high[...], p_low[...], vx_high[:, columns], vx_low[:, columns])
                high, low = split(lines)
                here = (pl.ds(r * grid_y + t * tile, tile), slice(b * 256, b * 256 + 256))
                g_high[here] = high
                g_low[here] = low
        return carry

    lax.fori_loop(0, grid_y // tile, middle, 0)
    per_step = min(count_y, max(1, 512 // pair))

    def back(i, carry):
        rows = pl.ds(i * per_step * pair, per_step * pair)
        for b in range(grid_x // 256):
            columns = slice(b * 256, b * 256 + 256)
            result = dot3(vy_high[rows, :], vy_low[rows, :], g_high[:, columns], g_low[:, columns])
            for h in range(256 // x_local):
                g = b * (256 // x_local) + h
                for j in range(per_step):
                    piece = result[j * pair : (j + 1) * pair, h * x_local : (h + 1) * x_local]
                    out_ref[g * count_y + i * per_step + j] = piece.reshape(2, 1, y_local, x_local)
        return carry

    lax.fori_loop(0, count_y // per_step, back, 0)


def plane_tile(grid_y):
    return min(256, grid_y)


def planes(received, tables, count_x, count_y, scale):
    devices, _, _, kz_chunk, y_local, x_local = received.shape
    grid_x, grid_y = count_x * x_local, count_y * y_local
    tile = plane_tile(grid_y)

    def whole(array):
        return pl.BlockSpec(array.shape, lambda i: (0, 0), pipeline_mode=pl.Buffered(1))

    flat_tables = [part for pair in tables for part in pair]

    def scratch(*shape):
        return [pltpu.VMEM(shape, jnp.bfloat16)] * 2

    def body(*refs):
        plane_kernel(*refs, count_x=count_x, count_y=count_y, tile=tile, scale=scale)

    return pl.pallas_call(
        body,
        grid=(kz_chunk,),
        in_specs=[
            pl.BlockSpec((devices, 2, 2, 1, y_local, x_local), lambda i: (0, 0, 0, i, 0, 0)),
            *[whole(part) for part in flat_tables],
        ],
        out_specs=pl.BlockSpec((devices, 2, 1, y_local, x_local), lambda i: (0, 0, i, 0, 0)),
        out_shape=jax.ShapeDtypeStruct((devices, 2, kz_chunk, y_local, x_local), jnp.float32),
        scratch_shapes=[
            *scratch(2, 2 * grid_y, grid_x),
            *scratch(2 * tile, 2 * grid_x),
            *scratch(tile, grid_x),
            *scratch(2 * grid_y, grid_x),
        ],
        compiler_params=pltpu.CompilerParams(vmem_limit_bytes=VMEM_LIMIT),
        name="planes",
    )(received, *flat_tables)


def plane_tables(anchor, grid_x, grid_y, count_y):
    y_local = grid_y // count_y
    tile = plane_tile(grid_y)

    def ids(length):
        return jnp.arange(length, dtype=jnp.int32) + anchor

    inner = ids(2 * grid_y)
    inner_y = inner // (2 * y_local) * y_local + inner % y_local
    inner_r = inner // y_local % 2
    outer_ky = inner // (2 * tile) * tile + inner % tile
    outer_r = inner // tile % 2
    wy = cosine_pair(
        outer_ky[:, None] * inner_y[None, :] + (outer_r[:, None] - inner_r[None, :] + 4) * (grid_y // 4), grid_y
    )
    plain = ids(2 * grid_x)
    plain_x, plain_r = plain % grid_x, plain // grid_x
    wx = cosine_pair(
        plain_x[:, None] * plain_x[None, :] + (plain_r[None, :] - plain_r[:, None] + 4) * (grid_x // 4), grid_x
    )
    vx = cosine_pair(ids(grid_x)[:, None] * plain_x[None, :] + (4 - plain_r[None, :]) * (grid_x // 4), grid_x)
    wave_y, wave_r = inner % grid_y, inner // grid_y
    vy = cosine_pair(
        inner_y[:, None] * wave_y[None, :] + (wave_r[None, :] - inner_r[:, None] + 4) * (grid_y // 4), grid_y
    )
    return wy, wx, vx, vy


def on_device(density_one, density_two):
    count_x = lax.axis_size("gx")
    count_y = lax.axis_size("gy")
    x_local, y_local, depth = density_one.shape
    grid_x, grid_y = x_local * count_x, y_local * count_y
    devices = count_x * count_y
    kz_slices = depth // 2 // devices
    chunks = MAX_CHUNKS if kz_slices % MAX_CHUNKS == 0 else 1
    kz_chunk = kz_slices // chunks
    rows = devices * 2 * kz_chunk
    fits = x_local % 128 == 0 and y_local % 8 == 0 and rows % 128 == 0 and 2 * kz_chunk % 8 == 0 and grid_x % 256 == 0 and grid_y % 256 == 0
    if not fits:
        return generic_device(density_one, density_two)
    cell_total = float(grid_x * grid_y * depth)
    cells = jnp.arange(depth, dtype=jnp.int32)
    rows_shape = (devices, 2, kz_chunk)

    def forward_table(chunk, anchor):
        wave, flag = depth_rows(chunk, chunks, devices, kz_slices)
        wave = wave + anchor
        return cosine_pair(cells[:, None] * wave[None, :] + flag[None, :] * (depth // 4), depth)

    def inverse_table(anchor):
        waves, flags = zip(*(depth_rows(chunk, chunks, devices, kz_slices) for chunk in range(chunks)))
        wave = jnp.concatenate(waves) + anchor
        flag = jnp.concatenate(flags)
        weight = jnp.where(wave == 0, 1.0, 2.0) * (1.0 / math.sqrt(cell_total))
        return cosine_pair(wave[:, None] * cells[None, :] + flag[:, None] * (depth // 4), depth, weight[:, None])

    zero = jnp.zeros((), jnp.int32)
    sent = [depth_forward(density_one, density_two, forward_table(0, zero), rows_shape)]
    sent[0], anchor = lax.optimization_barrier((sent[0], zero))
    for chunk in range(1, chunks):
        sent.append(depth_forward(density_one, density_two, forward_table(chunk, anchor), rows_shape))
    tables = plane_tables(anchor, grid_x, grid_y, count_y)
    back_table = inverse_table(anchor)
    back = []
    for chunk in range(chunks):
        moved = lax.all_to_all(sent[chunk], ("gx", "gy"), split_axis=0, concat_axis=0, tiled=True)
        lines = planes(moved, tables, count_x, count_y, 1.0 / cell_total)
        back.append(lax.all_to_all(lines, ("gx", "gy"), split_axis=0, concat_axis=0, tiled=True))
    return depth_inverse(back, back_table)


def solution(mesh):
    return jax.shard_map(
        on_device,
        mesh=mesh,
        in_specs=(P("gx", "gy", None), P("gx", "gy", None)),
        out_specs=P("gx", "gy", None),
        check_vma=False,
    )
```

```python
import math

import jax
import jax.numpy as jnp
from jax import lax
from jax.experimental import pallas as pl
from jax.experimental.pallas import tpu as pltpu
from jax.sharding import PartitionSpec as P

exact_mode = lax.Precision.HIGHEST


def phases(numerator, denominator):
    radians = (numerator % denominator).astype(jnp.float32) * (2.0 * math.pi / denominator)
    return (jnp.cos(radians), jnp.sin(radians))


def complex_table(length, direction):
    positions = jnp.arange(length, dtype=jnp.int32)
    cosines, sines_raw = phases(positions[:, None] * positions[None, :], length)
    signed = direction * sines_raw
    real_rows = jnp.stack([cosines, signed], axis=1)
    imag_rows = jnp.stack([-signed, cosines], axis=1)
    return jnp.stack([real_rows, imag_rows], axis=0)


def depth_tables(depth_cells, count_x, count_y):
    half_depth = depth_cells // 2
    kz_slices = half_depth // (count_x * count_y)
    row_ids = jnp.arange(2 * half_depth, dtype=jnp.int32)
    within = row_ids % kz_slices
    imag_flag = row_ids // kz_slices % 2
    row_block = row_ids // (2 * kz_slices)
    row_block = row_block % count_y * count_x + row_block // count_y
    wave_number = row_block * kz_slices + within
    cell_ids = jnp.arange(depth_cells, dtype=jnp.int32)
    cosines, sines_raw = phases(wave_number[:, None] * cell_ids[None, :], depth_cells)
    is_imag = (imag_flag == 1)[:, None]
    forward = jnp.where(is_imag, -sines_raw, cosines)
    weight = jnp.where(wave_number == 0, 1.0, 2.0)[:, None]
    inverse = jnp.where(is_imag, -weight * sines_raw, weight * cosines)
    return (forward, inverse)


def generic_device(density_one, density_two):
    count_x = lax.axis_size("gx")
    count_y = lax.axis_size("gy")
    x_local, y_local, depth_cells = density_one.shape
    grid_x = x_local * count_x
    grid_y = y_local * count_y
    kz_slices = depth_cells // 2 // (count_x * count_y)
    columns = x_local * y_local
    cell_total = float(grid_x * grid_y * depth_cells)
    forward_depth, inverse_depth = depth_tables(depth_cells, count_x, count_y)

    def depth_forward(density):
        flat_lines = density.reshape(columns, depth_cells)
        return lax.dot_general(
            forward_depth, flat_lines, (((1,), (1,)), ((), ())), precision=exact_mode
        )

    spectra = jnp.stack([depth_forward(density_one), depth_forward(density_two)])
    y_forward = complex_table(grid_y, -1.0).reshape(2, count_y, y_local, 2, grid_y)
    y_inverse = complex_table(grid_y, 1.0).reshape(2, grid_y, 2, count_y, y_local)
    block_forward = complex_table(count_x, -1.0)
    block_inverse = complex_table(count_x, 1.0)
    local_forward = complex_table(x_local, -1.0)
    sent = spectra.reshape(2, count_x * count_y, 2 * kz_slices, columns)
    moved = lax.all_to_all(sent, ("gx", "gy"), split_axis=1, concat_axis=1, tiled=True)
    moved = moved.reshape(2, count_x, count_y, 2, kz_slices, x_local, y_local)
    planes = jnp.einsum("fdspkjy,psyrq->fdrkjq", moved, y_forward, precision=exact_mode)
    aligned = jnp.einsum("fdpkjq,pdra->farkjq", planes, block_forward, precision=exact_mode)
    twiddle_cos, twiddle_sin = phases(
        jnp.arange(count_x, dtype=jnp.int32)[:, None]
        * jnp.arange(x_local, dtype=jnp.int32)[None, :],
        grid_x,
    )
    forward_cos = twiddle_cos[None, :, None, :, None]
    forward_sin = twiddle_sin[None, :, None, :, None]
    real_part = aligned[:, :, 0]
    imag_part = aligned[:, :, 1]
    turned = jnp.stack(
        [
            real_part * forward_cos + imag_part * forward_sin,
            imag_part * forward_cos - real_part * forward_sin,
        ],
        axis=2,
    )
    spectra_k = jnp.einsum("fapkjq,pjrb->farkbq", turned, local_forward, precision=exact_mode)
    power = (
        spectra_k[0, :, 0] * spectra_k[1, :, 0] + spectra_k[0, :, 1] * spectra_k[1, :, 1]
    ) / cell_total
    wave_x = (
        jnp.arange(count_x, dtype=jnp.int32)[:, None]
        + count_x * jnp.arange(x_local, dtype=jnp.int32)[None, :]
    )
    keep_x = (wave_x != grid_x // 2)[:, None, :, None]
    keep_y = (jnp.arange(grid_y, dtype=jnp.int32) != grid_y // 2)[None, None, None, :]
    power = jnp.where(keep_x & keep_y, power, 0.0)
    cos_local, sin_local = phases(
        jnp.arange(x_local, dtype=jnp.int32)[:, None]
        * jnp.arange(x_local, dtype=jnp.int32)[None, :],
        x_local,
    )
    real_table = jnp.stack([cos_local, sin_local], axis=1)
    lines = jnp.einsum("akbq,brj->arkjq", power, real_table, precision=exact_mode)
    inverse_cos = twiddle_cos[:, None, :, None]
    inverse_sin = twiddle_sin[:, None, :, None]
    real_part = lines[:, 0]
    imag_part = lines[:, 1]
    unturned = jnp.stack(
        [
            real_part * inverse_cos - imag_part * inverse_sin,
            imag_part * inverse_cos + real_part * inverse_sin,
        ],
        axis=1,
    )[None]
    blocks = jnp.einsum("fapkjq,pard->fdrkjq", unturned, block_inverse, precision=exact_mode)
    back_lines = jnp.einsum("fdpkjq,pqrsy->fdsrkjy", blocks, y_inverse, precision=exact_mode)
    sent_back = back_lines.reshape(1, count_x * count_y, 2 * kz_slices, columns)
    rows_back = lax.all_to_all(sent_back, ("gx", "gy"), split_axis=1, concat_axis=1, tiled=True)
    rows_flat = rows_back.reshape(2 * kz_slices * count_x * count_y, columns)
    correlation = lax.dot_general(
        rows_flat, inverse_depth, (((0,), (0,)), ((), ())), precision=exact_mode
    )
    correlation = correlation * (1.0 / math.sqrt(cell_total))
    return correlation.reshape(x_local, y_local, depth_cells)


VMEM_LIMIT = 60 * 1024 * 1024
Y_BLOCK = 8


def split(value):
    high = value.astype(jnp.bfloat16)
    low = (value - high.astype(jnp.float32)).astype(jnp.bfloat16)
    return high, low


def dot3(left_high, left_low, right_high, right_low):
    def one(a, b):
        return jnp.dot(a, b, preferred_element_type=jnp.float32)

    return one(left_high, right_high) + one(left_high, right_low) + one(left_low, right_high)


def cosine_pair(steps, length, factor=None):
    turned = jnp.cos((steps % length).astype(jnp.float32) * (2.0 * math.pi / length))
    if factor is not None:
        turned = turned * factor
    high = lax.reduce_precision(turned, 8, 7)
    return high.astype(jnp.bfloat16), (turned - high).astype(jnp.bfloat16)


def depth_rows(chunk, devices, kz_slices):
    per_chunk = kz_slices // 2
    rows = jnp.arange(devices * 2 * per_chunk, dtype=jnp.int32)
    device = rows // (2 * per_chunk)
    flag = rows // per_chunk % 2
    return device * kz_slices + rows % per_chunk * 2 + chunk, flag


def depth_forward_kernel(one_ref, two_ref, high_ref, low_ref, out_ref, *turn_refs, sign):
    x_local, y_block, depth = one_ref.shape
    rows = high_ref.shape[1]
    lines = x_local * y_block
    group = out_ref.shape[2] * out_ref.shape[3]
    flat_out = out_ref.reshape(2 * rows * y_block, x_local)
    for field, ref in enumerate((one_ref, two_ref)):
        flat = ref.reshape(lines, depth)
        near, far = flat[:, : depth // 2], flat[:, depth // 2 :]
        high, low = split(near + far if sign > 0 else near - far)
        product = dot3(high, low, high_ref[...], low_ref[...])
        for part in range(rows // 128):
            lanes = turn_refs[field * (rows // 128) + part]
            lanes[...] = product[:, part * 128 : part * 128 + 128]
            for j in range(y_block):
                turned = lanes[pl.ds(j, x_local, stride=y_block), :].T
                for d in range(128 // group):
                    start = (2 * (part * (128 // group) + d) + field) * group * y_block + j
                    flat_out[pl.ds(start, group, stride=y_block), :] = turned[d * group : d * group + group]


def depth_forward(one, two, table, rows_shape, sign):
    x_local, y_local, depth = one.shape
    rows = math.prod(rows_shape)
    out_rows = (rows_shape[0], 2, *rows_shape[1:])
    field_spec = pl.BlockSpec((x_local, Y_BLOCK, depth), lambda i: (0, i, 0))
    table_spec = pl.BlockSpec((depth // 2, rows), lambda i: (0, 0))

    def body(*refs):
        depth_forward_kernel(*refs, sign=sign)

    return pl.pallas_call(
        body,
        grid=(y_local // Y_BLOCK,),
        in_specs=[field_spec, field_spec, table_spec, table_spec],
        out_specs=pl.BlockSpec((*out_rows, Y_BLOCK, x_local), lambda i: (0, 0, 0, 0, i, 0)),
        out_shape=jax.ShapeDtypeStruct((*out_rows, y_local, x_local), jnp.float32),
        scratch_shapes=[pltpu.VMEM((x_local * Y_BLOCK, 128), jnp.float32)] * (2 * rows // 128),
        compiler_params=pltpu.CompilerParams(vmem_limit_bytes=VMEM_LIMIT),
        name="depth_forward",
    )(one, two, *table)


def depth_inverse_kernel(even_ref, odd_ref, even_high, even_low, odd_high, odd_low, out_ref, *turn_refs):
    x_local, y_block, depth = out_ref.shape
    lines = x_local * y_block
    rows = even_high.shape[0]
    sums = []
    for p, (part_ref, high_ref, low_ref) in enumerate(
        ((even_ref, even_high, even_low), (odd_ref, odd_high, odd_low))
    ):
        flat = part_ref.reshape(rows * y_block, x_local)
        turns = turn_refs[p * (rows // 128) : (p + 1) * (rows // 128)]
        for part, turn in enumerate(turns):
            for j in range(y_block):
                block = flat[pl.ds(part * 128 * y_block + j, 128, stride=y_block), :]
                turn[pl.ds(j, x_local, stride=y_block), :] = block.T
        high, low = split(jnp.concatenate([turn[...] for turn in turns], axis=1))
        sums.append(dot3(high, low, high_ref[...], low_ref[...]))
    flat_out = out_ref.reshape(lines, depth)
    flat_out[:, : depth // 2] = sums[0] + sums[1]
    flat_out[:, depth // 2 :] = sums[0] - sums[1]


def depth_inverse(parts, tables):
    devices, two, kz_chunk, y_local, x_local = parts[0].shape
    rows, half = tables[0][0].shape
    part_spec = pl.BlockSpec((devices, two, kz_chunk, Y_BLOCK, x_local), lambda i: (0, 0, 0, i, 0))
    table_spec = pl.BlockSpec((rows, half), lambda i: (0, 0))
    return pl.pallas_call(
        depth_inverse_kernel,
        grid=(y_local // Y_BLOCK,),
        in_specs=[part_spec] * 2 + [table_spec] * 4,
        out_specs=pl.BlockSpec((x_local, Y_BLOCK, 2 * half), lambda i: (0, i, 0)),
        out_shape=jax.ShapeDtypeStruct((x_local, y_local, 2 * half), jnp.float32),
        scratch_shapes=[pltpu.VMEM((x_local * Y_BLOCK, 128), jnp.float32)] * (2 * rows // 128),
        compiler_params=pltpu.CompilerParams(vmem_limit_bytes=VMEM_LIMIT),
        name="depth_inverse",
    )(*parts, *tables[0], *tables[1])


def plane_kernel(
    s_ref, wy_high, wy_low, wx_high, wx_low, vx_high, vx_low, vy_high, vy_low, out_ref,
    s_high, s_low, y_high, y_low, p_high, p_low, g_high, g_low, *, count_x, count_y, tile, scale,
):
    y_local, x_local = out_ref.shape[-2:]
    grid_x, grid_y = count_x * x_local, count_y * y_local
    pair = 2 * y_local

    def load(i, carry):
        field, row = i // count_y, i % count_y
        for g in range(count_x):
            values = s_ref[g * count_y + row, field].reshape(pair, x_local)
            high, low = split(values)
            here = (field, pl.ds(row * pair, pair), slice(g * x_local, (g + 1) * x_local))
            s_high[here] = high
            s_low[here] = low
        return carry

    lax.fori_loop(0, 2 * count_y, load, 0)

    def middle(t, carry):
        rows = pl.ds(t * 2 * tile, 2 * tile)
        for field in range(2):
            for b in range(grid_x // 256):
                columns = slice(b * 256, b * 256 + 256)
                planes = dot3(
                    wy_high[rows, :], wy_low[rows, :], s_high[field, :, columns], s_low[field, :, columns]
                )
                high, low = split(planes)
                for r in range(2):
                    lanes = slice(r * grid_x + b * 256, r * grid_x + b * 256 + 256)
                    y_high[field * tile : (field + 1) * tile, lanes] = high[r * tile : (r + 1) * tile]
                    y_low[field * tile : (field + 1) * tile, lanes] = low[r * tile : (r + 1) * tile]
        for b in range(grid_x // 256):
            power = None
            for r in range(2):
                columns = slice(r * grid_x + b * 256, r * grid_x + b * 256 + 256)
                z = dot3(y_high[...], y_low[...], wx_high[:, columns], wx_low[:, columns])
                term = z[:tile] * z[tile:]
                power = term if power is None else power + term
            wave_y = t * tile + lax.broadcasted_iota(jnp.int32, power.shape, 0)
            wave_x = b * 256 + lax.broadcasted_iota(jnp.int32, power.shape, 1)
            keep = (wave_x != grid_x // 2) & (wave_y != grid_y // 2)
            high, low = split(jnp.where(keep, power * scale, 0.0))
            p_high[:, b * 256 : b * 256 + 256] = high
            p_low[:, b * 256 : b * 256 + 256] = low
        for r in range(2):
            for b in range(grid_x // 256):
                columns = slice(r * grid_x + b * 256, r * grid_x + b * 256 + 256)
                lines = dot3(p_high[...], p_low[...], vx_high[:, columns], vx_low[:, columns])
                high, low = split(lines)
                here = (pl.ds(r * grid_y + t * tile, tile), slice(b * 256, b * 256 + 256))
                g_high[here] = high
                g_low[here] = low
        return carry

    lax.fori_loop(0, grid_y // tile, middle, 0)
    per_step = min(count_y, max(1, 512 // pair))

    def back(i, carry):
        rows = pl.ds(i * per_step * pair, per_step * pair)
        for b in range(grid_x // 256):
            columns = slice(b * 256, b * 256 + 256)
            result = dot3(vy_high[rows, :], vy_low[rows, :], g_high[:, columns], g_low[:, columns])
            for h in range(256 // x_local):
                g = b * (256 // x_local) + h
                for j in range(per_step):
                    piece = result[j * pair : (j + 1) * pair, h * x_local : (h + 1) * x_local]
                    out_ref[g * count_y + i * per_step + j] = piece.reshape(2, 1, y_local, x_local)
        return carry

    lax.fori_loop(0, count_y // per_step, back, 0)


def plane_tile(grid_y):
    return min(256, grid_y)


def planes(received, tables, count_x, count_y, scale):
    devices, _, _, kz_chunk, y_local, x_local = received.shape
    grid_x, grid_y = count_x * x_local, count_y * y_local
    tile = plane_tile(grid_y)

    def whole(array):
        return pl.BlockSpec(array.shape, lambda i: (0, 0), pipeline_mode=pl.Buffered(1))

    flat_tables = [part for pair in tables for part in pair]

    def scratch(*shape):
        return [pltpu.VMEM(shape, jnp.bfloat16)] * 2

    def body(*refs):
        plane_kernel(*refs, count_x=count_x, count_y=count_y, tile=tile, scale=scale)

    return pl.pallas_call(
        body,
        grid=(kz_chunk,),
        in_specs=[
            pl.BlockSpec((devices, 2, 2, 1, y_local, x_local), lambda i: (0, 0, 0, i, 0, 0)),
            *[whole(part) for part in flat_tables],
        ],
        out_specs=pl.BlockSpec((devices, 2, 1, y_local, x_local), lambda i: (0, 0, i, 0, 0)),
        out_shape=jax.ShapeDtypeStruct((devices, 2, kz_chunk, y_local, x_local), jnp.float32),
        scratch_shapes=[
            *scratch(2, 2 * grid_y, grid_x),
            *scratch(2 * tile, 2 * grid_x),
            *scratch(tile, grid_x),
            *scratch(2 * grid_y, grid_x),
        ],
        compiler_params=pltpu.CompilerParams(vmem_limit_bytes=VMEM_LIMIT),
        name="planes",
    )(received, *flat_tables)


def plane_tables(anchor, grid_x, grid_y, count_y):
    y_local = grid_y // count_y
    tile = plane_tile(grid_y)

    def ids(length):
        return jnp.arange(length, dtype=jnp.int32) + anchor

    inner = ids(2 * grid_y)
    inner_y = inner // (2 * y_local) * y_local + inner % y_local
    inner_r = inner // y_local % 2
    outer_ky = inner // (2 * tile) * tile + inner % tile
    outer_r = inner // tile % 2
    wy = cosine_pair(
        outer_ky[:, None] * inner_y[None, :] + (outer_r[:, None] - inner_r[None, :] + 4) * (grid_y // 4), grid_y
    )
    plain = ids(2 * grid_x)
    plain_x, plain_r = plain % grid_x, plain // grid_x
    wx = cosine_pair(
        plain_x[:, None] * plain_x[None, :] + (plain_r[None, :] - plain_r[:, None] + 4) * (grid_x // 4), grid_x
    )
    vx = cosine_pair(ids(grid_x)[:, None] * plain_x[None, :] + (4 - plain_r[None, :]) * (grid_x // 4), grid_x)
    wave_y, wave_r = inner % grid_y, inner // grid_y
    vy = cosine_pair(
        inner_y[:, None] * wave_y[None, :] + (wave_r[None, :] - inner_r[:, None] + 4) * (grid_y // 4), grid_y
    )
    return wy, wx, vx, vy


def on_device(density_one, density_two):
    count_x = lax.axis_size("gx")
    count_y = lax.axis_size("gy")
    x_local, y_local, depth = density_one.shape
    grid_x, grid_y = x_local * count_x, y_local * count_y
    devices = count_x * count_y
    kz_slices = depth // 2 // devices
    kz_chunk = kz_slices // 2
    rows = devices * 2 * kz_chunk
    fits = x_local % 128 == 0 and y_local % 8 == 0 and grid_x % 256 == 0 and grid_y % 256 == 0
    fits = fits and kz_slices % 8 == 0 and rows % 128 == 0 and depth % 256 == 0
    if not fits:
        return generic_device(density_one, density_two)
    cell_total = float(grid_x * grid_y * depth)
    cells = jnp.arange(depth // 2, dtype=jnp.int32)
    rows_shape = (devices, 2, kz_chunk)

    def forward_table(chunk, anchor):
        wave, flag = depth_rows(chunk, devices, kz_slices)
        wave = wave + anchor
        return cosine_pair(cells[:, None] * wave[None, :] + flag[None, :] * (depth // 4), depth)

    def inverse_table(chunk, anchor):
        wave, flag = depth_rows(chunk, devices, kz_slices)
        wave = wave + anchor
        weight = jnp.where(wave == 0, 1.0, 2.0) * (1.0 / math.sqrt(cell_total))
        return cosine_pair(wave[:, None] * cells[None, :] + flag[:, None] * (depth // 4), depth, weight[:, None])

    zero = jnp.zeros((), jnp.int32)
    even = depth_forward(density_one, density_two, forward_table(0, zero), rows_shape, 1)
    even, anchor = lax.optimization_barrier((even, zero))
    odd = depth_forward(density_one, density_two, forward_table(1, anchor), rows_shape, -1)
    tables = plane_tables(anchor, grid_x, grid_y, count_y)
    back_tables = [inverse_table(chunk, anchor) for chunk in range(2)]
    back = []
    for sent in (even, odd):
        moved = lax.all_to_all(sent, ("gx", "gy"), split_axis=0, concat_axis=0, tiled=True)
        lines = planes(moved, tables, count_x, count_y, 1.0 / cell_total)
        back.append(lax.all_to_all(lines, ("gx", "gy"), split_axis=0, concat_axis=0, tiled=True))
    return depth_inverse(back, back_tables)


def solution(mesh):
    return jax.shard_map(
        on_device,
        mesh=mesh,
        in_specs=(P("gx", "gy", None), P("gx", "gy", None)),
        out_specs=P("gx", "gy", None),
        check_vma=False,
    )
```
